64 devices in a mesh: dp: 8 (over x, y, core), sp: 8 (over z).
Axes of the slice: x: 2, y: 2, z: 8, core: 2. Of those that a mesh axis runs over, the one named last changes fastest.
The devices are a block of a 4x4x8 slice.
Arguments:
- x: bfloat16 [16384, 7168], P(('dp', 'sp')), parts along dimension 0
- gain: bfloat16 [7168], replicated
- wq: bfloat16 [7168, 7168], replicated
- wk: bfloat16 [7168, 7168], replicated
- wv: bfloat16 [7168, 7168], replicated
- wo: bfloat16 [7168, 7168], replicated
Outputs:
- output: bfloat16 [16384, 7168], P(('dp', 'sp')), parts along dimension 0
There are 8 independent parts. The reference program is written for one: setup_inputs(seed, part) draws one part's arguments, and reference() takes and returns one part's arrays. A program takes and returns all parts, laid end to end along the dimension named above; an argument that names none is the same for every part.
All inputs are finite; a program needn't handle non-finite values.
Results may differ from the reference program's by a relative error of at most 0.012.
Values are sent between devices in bfloat16 or wider.
A program may use at most 768 MiB of HBM per device.

```python
import jax
import jax.numpy as jnp
from jax import lax

ROWS = 2048
D = 7168
HEADS = 56
KV_HEADS = 56
HEAD = 128
THETA = 10000


def setup_inputs(seed: int = 0, part: int = 0) -> dict:
    kx, kn, kq, kk, kv, ko = jax.random.split(jax.random.key(seed), 6)

    def weights(key, rows, columns):
        return jax.random.normal(key, (rows, columns), jnp.float32) * rows**-0.5

    drawn = {
        "x": jax.random.normal(jax.random.fold_in(kx, part), (ROWS, D), jnp.float32),
        "gain": 1 + 0.1 * jax.random.normal(kn, (D,), jnp.float32),
        "wq": 2 * weights(kq, D, HEADS * HEAD),
        "wk": 2 * weights(kk, D, KV_HEADS * HEAD),
        "wv": 4 * weights(kv, D, KV_HEADS * HEAD),
        "wo": weights(ko, HEADS * HEAD, D),
    }
    return {k: v.astype(jnp.bfloat16) for k, v in drawn.items()}


def normed(x, gain):
    wide = x.astype(jnp.float32)
    scale = lax.rsqrt(jnp.mean(wide * wide, -1, keepdims=True) + 1e-6)
    return (wide * scale * gain.astype(jnp.float32)).astype(jnp.bfloat16)


def turned(t, place, theta):
    half = t.shape[-1] // 2
    angle = place.astype(jnp.float32)[:, None] * theta ** (-jnp.arange(half, dtype=jnp.float32) / half)
    cos, sin = jnp.cos(angle)[:, None], jnp.sin(angle)[:, None]
    a, b = t[..., :half].astype(jnp.float32), t[..., half:].astype(jnp.float32)
    return jnp.concatenate([a * cos - b * sin, b * cos + a * sin], -1).astype(jnp.bfloat16)


def matmul(a, w):
    return jnp.dot(a, w, preferred_element_type=jnp.float32).astype(jnp.bfloat16)


def einsum(form, a, b):
    return jnp.einsum(form, a.astype(jnp.float32), b.astype(jnp.float32))


def attention(q, k, v):
    scores = einsum("tgsd,ugd->gstu", q, k) * q.shape[-1] ** -0.5
    token = jnp.arange(q.shape[0])
    scores = jnp.where(token[:, None] >= token, scores, -jnp.inf)
    weights = jax.nn.softmax(scores, -1).astype(jnp.bfloat16)
    return einsum("gstu,ugd->tgsd", weights, v).astype(jnp.bfloat16)


def reference(x, gain, wq, wk, wv, wo):
    a, place = normed(x, gain), jnp.arange(ROWS)
    q = turned(matmul(a, wq).reshape(ROWS, HEADS, HEAD), place, THETA).reshape(ROWS, KV_HEADS, -1, HEAD)
    k = turned(matmul(a, wk).reshape(ROWS, KV_HEADS, HEAD), place, THETA)
    v = matmul(a, wv).reshape(ROWS, KV_HEADS, HEAD)
    seen = attention(q, k, v).reshape(ROWS, HEADS * HEAD)
    return (x.astype(jnp.float32) + jnp.dot(seen, wo, preferred_element_type=jnp.float32)).astype(jnp.bfloat16)
```

```python
import functools

import jax
import jax.numpy as jnp
from jax import lax
from jax.experimental import pallas as pl
from jax.experimental.pallas import tpu as pltpu
from jax.sharding import PartitionSpec as P

HEAD = 128
THETA = 10000
TILE = 256
SLOTS = 3
STRIP = 512
LOG2E = 1.4426950408889634
NEG = -1e30
MESH = pl.DeviceIdType.MESH


def _dot(a, b, ca, cb):
    return lax.dot_general(a, b, (((ca,), (cb,)), ((), ())), preferred_element_type=jnp.float32)


def _kernel(n, rounds, x_hbm, gain_ref, cos_ref, sin_ref, wq, wk, wv, wo, out_hbm,
            a, wbuf, stage, recv, ostage, orecv, y, mix, top,
            wsem, xsem, ssem, rsem, ossem, orsem, outsem):
    own, d = a.shape
    me = lax.axis_index("sp")
    per = n * HEAD // TILE
    two = TILE // HEAD
    steps = rounds * per * 3
    group = n * HEAD
    parts = d // group
    osteps = d // (parts * TILE)
    total = steps + rounds * osteps
    to = lambda p: {"sp": p}

    barrier = pltpu.get_barrier_semaphore()
    for k in range(1, n):
        pl.semaphore_signal(barrier, inc=1, device_id=to(lax.rem(me + k, n)), device_id_type=MESH)

    def where(s):
        r, m = lax.div(s, 3 * per), lax.rem(s, 3 * per)
        kind, t = lax.div(m, per), lax.rem(lax.rem(m, per) + lax.div(me, two), per)
        return r, kind, t

    def load(s):
        slot = lax.rem(s, SLOTS)

        @pl.when(s < steps)
        def _():
            r, kind, t = where(s)
            cols = pl.ds(pl.multiple_of((r * per + t) * TILE, TILE), TILE)
            for i, w in enumerate((wk, wv, wq)):
                @pl.when(kind == i)
                def _():
                    pltpu.make_async_copy(w.at[:, cols], wbuf.at[slot], wsem.at[slot]).start()

        @pl.when((s >= steps) & (s < total))
        def _():
            r, m = lax.div(s - steps, osteps), lax.rem(s - steps, osteps)
            rows = pl.ds(pl.multiple_of(r * group, group), group)
            for c in range(parts):
                cols = pl.ds(pl.multiple_of((m * parts + c) * TILE, TILE), TILE)
                pltpu.make_async_copy(wo.at[rows, cols], wbuf.at[slot, pl.ds(c * group, group)], wsem.at[slot]).start()

    def loaded(s):
        slot = lax.rem(s, SLOTS)
        pltpu.make_async_copy(wbuf.at[slot], wbuf.at[slot], wsem.at[slot]).wait()
        return slot

    getx = pltpu.make_async_copy(x_hbm, a, xsem)
    getx.start()
    for s in range(SLOTS - 1):
        load(jnp.int32(s))
    getx.wait()

    chunk = 16
    gain = gain_ref[...].astype(jnp.float32)

    def norm(i, _):
        rows = pl.ds(pl.multiple_of(i * chunk, chunk), chunk)
        wide = a[rows, :].astype(jnp.float32)
        scale = lax.rsqrt(jnp.mean(wide * wide, -1, keepdims=True) + 1e-6)
        a[rows, :] = (wide * scale * gain).astype(jnp.bfloat16)
        return 0

    lax.fori_loop(0, own // chunk, norm, 0)
    pl.semaphore_wait(barrier, n - 1)

    def send(s):
        r, kind, t = where(s)
        for h in range(two):
            p = t * two + h

            @pl.when(p != me)
            def _():
                pltpu.make_async_remote_copy(
                    src_ref=stage.at[r, kind * n + p], dst_ref=recv.at[r, kind * n + me], send_sem=ssem.at[r], recv_sem=rsem.at[r],
                    device_id=to(p), device_id_type=MESH).start()

    def project(s, _):
        load(s + SLOTS - 1)
        slot = loaded(s)

        @pl.when(s > 0)
        def _():
            send(s - 1)

        r, kind, t = where(s)
        got = _dot(a[...], wbuf[slot], 1, 0)

        def keep(h, val):
            p = t * two + h
            stage[r, kind * n + p] = val

            @pl.when(p == me)
            def _():
                recv[r, kind * n + me] = val

        for h in range(two):
            val = got[:, h * HEAD : (h + 1) * HEAD].astype(jnp.bfloat16)

            @pl.when(kind == 1)
            def _():
                keep(h, val)

            @pl.when(kind != 1)
            def _():
                f = val.astype(jnp.float32)
                keep(h, (f * cos_ref[...] + pltpu.roll(f, HEAD // 2, 1) * sin_ref[...]).astype(jnp.bfloat16))

        return 0

    lax.fori_loop(0, steps, project, 0)
    send(jnp.int32(steps - 1))

    again = pltpu.make_async_copy(x_hbm, a, xsem)
    again.start()
    y[...] = jnp.zeros_like(y)

    e = HEAD**-0.5 * LOG2E
    strips = n * own // STRIP
    blocks = STRIP // own
    ones = jnp.ones((8, STRIP), jnp.bfloat16)

    def attend(r, _):
        got = recv.at[r, pl.ds(0, 3 * (n - 1))]
        pltpu.make_async_copy(got, got, rsem.at[r]).wait()
        pick = lambda kind, i: recv[r, pl.ds(kind * n + i * blocks, blocks)].reshape(STRIP, HEAD)
        for j in range(strips):
            keys = pick(0, j)
            values = jnp.concatenate([pick(1, j).T, ones], axis=0)
            scores = [_dot(keys, pick(2, i), 1, 1) for i in range(j, strips)]
            weights, keeps = [], []
            for i, s in zip(range(j, strips), scores):
                cols = pl.ds(i * STRIP, STRIP)
                if i == j:
                    seen = lax.broadcasted_iota(jnp.int32, s.shape, 1) >= lax.broadcasted_iota(jnp.int32, s.shape, 0)
                    s = jnp.where(seen, s, NEG)
                best = s.max(axis=0, keepdims=True)
                if j:
                    old = top[:, cols]
                    best = jnp.maximum(old, best)
                    keeps.append(jnp.exp2((old - best) * e))
                if i > j:
                    top[:, cols] = best
                weights.append(jnp.exp2((s - best) * e).astype(jnp.bfloat16))
            for c, (i, p) in enumerate(zip(range(j, strips), weights)):
                cols = pl.ds(i * STRIP, STRIP)
                new = _dot(values, p, 1, 0)
                if j:
                    new += mix[:, cols] * keeps[c]
                if i > j:
                    mix[:, cols] = new
                else:
                    out = (new[:HEAD] * (1 / new[HEAD : HEAD + 1])).T.astype(jnp.bfloat16)
                    for b in range(blocks):
                        owner = i * blocks + b
                        part = out[b * own : (b + 1) * own]
                        ostage[r, owner] = part

                        @pl.when(owner == me)
                        def _():
                            orecv[r, :, pl.ds(pl.multiple_of(me * HEAD, HEAD), HEAD)] = part

        for owner in range(n):
            @pl.when(owner != me)
            def _():
                pltpu.make_async_remote_copy(
                    src_ref=ostage.at[r, owner], dst_ref=orecv.at[r, :, pl.ds(pl.multiple_of(me * HEAD, HEAD), HEAD)],
                    send_sem=ossem.at[r], recv_sem=orsem.at[r], device_id=to(owner), device_id_type=MESH).start()
        return 0

    lax.fori_loop(0, rounds, attend, 0)
    again.wait()

    def output(s, _):
        r, m = lax.div(s, osteps), lax.rem(s, osteps)
        load(steps + s + SLOTS - 1)
        slot = loaded(steps + s)

        @pl.when(m == 0)
        def _():
            got = orecv.at[r, :, pl.ds(0, (n - 1) * HEAD)]
            pltpu.make_async_copy(got, got, orsem.at[r]).wait()

        for c in range(parts):
            cols = pl.ds(pl.multiple_of((m * parts + c) * TILE, TILE), TILE)
            y[:, cols] += _dot(orecv[r], wbuf[slot, c * group : (c + 1) * group], 1, 0)

        @pl.when(r == rounds - 1)
        def _():
            cols = pl.ds(pl.multiple_of(m * parts * TILE, TILE), parts * TILE)
            a[:, cols] = (a[:, cols].astype(jnp.float32) + y[:, cols]).astype(jnp.bfloat16)

            @pl.when(m > 0)
            def _():
                before = pl.ds(pl.multiple_of((m - 1) * parts * TILE, TILE), parts * TILE)
                pltpu.make_async_copy(a.at[:, before], out_hbm.at[:, before], outsem).start()

        return 0

    lax.fori_loop(0, rounds * osteps, output, 0)
    rest = pl.ds((osteps - 1) * parts * TILE, parts * TILE)
    pltpu.make_async_copy(a.at[:, rest], out_hbm.at[:, rest], outsem).start()
    for r in range(rounds):
        sent = stage.at[r, pl.ds(0, 3 * (n - 1))]
        pltpu.make_async_copy(sent, sent, ssem.at[r]).wait()
        sent = ostage.at[r, pl.ds(0, n - 1)]
        pltpu.make_async_copy(sent, sent, ossem.at[r]).wait()
    pltpu.make_async_copy(a, out_hbm, outsem).wait()


def solution(mesh):
    n = mesh.shape["sp"]

    def step(x, gain, wq, wk, wv, wo):
        own, d = x.shape
        rounds = wq.shape[1] // (n * HEAD)
        half = HEAD // 2
        place = lax.axis_index("sp") * own + jnp.arange(own)
        angle = place.astype(jnp.float32)[:, None] * THETA ** (-jnp.arange(half, dtype=jnp.float32) / half)
        cos, sin = jnp.cos(angle), jnp.sin(angle)
        cos, sin = jnp.concatenate([cos, cos], -1), jnp.concatenate([-sin, sin], -1)
        hbm, vmem = pl.BlockSpec(memory_space=pl.ANY), pl.BlockSpec(memory_space=pltpu.VMEM)
        bf16, f32 = jnp.bfloat16, jnp.float32
        dma = pltpu.SemaphoreType.DMA
        return pl.pallas_call(
            functools.partial(_kernel, n, rounds),
            name="layer",
            out_shape=jax.ShapeDtypeStruct((own, d), bf16),
            in_specs=[hbm, vmem, vmem, vmem, hbm, hbm, hbm, hbm],
            out_specs=hbm,
            scratch_shapes=[
                pltpu.VMEM((own, d), bf16),
                pltpu.VMEM((SLOTS, d, TILE), bf16),
                pltpu.VMEM((rounds, 3 * n, own, HEAD), bf16),
                pltpu.VMEM((rounds, 3 * n, own, HEAD), bf16),
                pltpu.VMEM((rounds, n, own, HEAD), bf16),
                pltpu.VMEM((rounds, own, n * HEAD), bf16),
                pltpu.VMEM((own, d), f32),
                pltpu.VMEM((HEAD + 8, n * own), f32),
                pltpu.VMEM((1, n * own), f32),
                dma((SLOTS,)), dma, dma((rounds,)), dma((rounds,)), dma((rounds,)), dma((rounds,)), dma,
            ],
            compiler_params=pltpu.CompilerParams(collective_id=0, has_side_effects=True, vmem_limit_bytes=67043328),
        )(x, gain[None], cos, sin, wq, wk, wv, wo)

    tokens, whole = P(("dp", "sp"), None), P(None, None)
    return jax.shard_map(
        step,
        mesh=mesh,
        in_specs=(tokens, P(None), whole, whole, whole, whole),
        out_specs=tokens,
        check_vma=False,
    )
```

```python
import functools

import jax
import jax.numpy as jnp
from jax import lax
from jax.experimental import pallas as pl
from jax.experimental.pallas import tpu as pltpu
from jax.sharding import PartitionSpec as P

HEAD = 128
THETA = 10000
TWO = 2
TILE = TWO * HEAD
LAG = 10
BACK = 16
KEPT = BACK - LAG + 1
LATE = 6
LOG2E = 1.4426950408889634
NEG = -1e30
MESH = pl.DeviceIdType.MESH

PLACES = (
    (0o40004222222221, 0o4440004440004),
    (0o22222222222220, 0o66222226222222),
    (0o44664466466111, 0o66444666444664),
    (0o11111111111111, 0o66111116111111),
    (0o33333333333330, 0o77333336333333),
    (0o47774777777111, 0o74447774447774),
    (0o33333333333330, 0o66333336333333),
    (0o3222222220, 0o55500005500005),
    (0o55555555555111, 0o75555555555555),
    (0o33333333333330, 0o73333333333333),
    (0o40004222222220, 0o4440004440004),
    (0o55555555555111, 0o55555555555555),
    (0o2222222220, 0o0),
    (0o44774477411111, 0o74444774444774),
)
ORDER = (0, 6, 3, 8, 10, 5, 1, 6, 8, 3, 4, 5, 1, 7, 2, 6, 3, 5, 1, 11, 6, 13, 12, 3, 11, 9, 1, 5)


class Plan:
    def __init__(self, n):
        self.jobs = []
        for first, second in PLACES:
            code = first + (second << 42)
            jobs = [[1 << j if j == d else 0 for d in range(n)] for j in range(n)]
            for j in range(1, n):
                for i in range(j):
                    jobs[j][code % 8] |= 1 << i
                    code //= 8
            self.jobs.append(jobs)
        kinds, devs = range(len(PLACES)), range(n)
        bits = lambda test: sum(1 << x for x in devs if test(x))
        need = lambda c, d, i: i != d and any(self.jobs[c][j][d] >> i & 1 for j in devs)
        away = lambda c, d, j: j != d and self.jobs[c][j][d] != 0
        self.kv_to = [[bits(lambda d: need(c, d, i)) for i in devs] for c in kinds]
        self.kv_from = [[bits(lambda i: need(c, d, i)) for d in devs] for c in kinds]
        self.q_to = [[bits(lambda d: away(c, d, j)) for j in devs] for c in kinds]
        self.q_from = [[bits(lambda j: away(c, d, j)) for d in devs] for c in kinds]
        self.most = max(bin(b).count("1") for row in self.q_to for b in row)
        rank = lambda c, d, j: bin(self.q_to[c][j] & ((1 << d) - 1)).count("1")
        held = [[bin(self.q_from[ORDER[u]][d]).count("1") for d in devs] for u in range(len(ORDER))]
        self.start = [[sum(row[d] for row in held[:u]) for d in devs] for u in range(len(ORDER))]
        self.held = max(sum(row[d] for row in held) for d in devs)
        self.place = [[[bits(lambda j: away(c, d, j) and rank(c, d, j) >> b & 1) for d in devs] for c in kinds] for b in range(2)]


def _dot(a, b, ca, cb):
    return lax.dot_general(a, b, (((ca,), (cb,)), ((), ())), preferred_element_type=jnp.float32)


def _choose(index, values):
    out = jnp.int32(values[0])
    for i, v in enumerate(values[1:], 1):
        out = jnp.where(index == i, v, out)
    return out


def _first(tests):
    out = jnp.int32(0)
    for i in range(len(tests) - 1, -1, -1):
        out = jnp.where(tests[i], i, out)
    return out


def _signed(x):
    return jnp.int32(x - (1 << 32) if x >> 31 else x)


def _kernel(n, units, plan, x_hbm, gain_ref, cos_ref, sin_ref, wq, wk, wv, wo, a, kvrecv, qrecv,
            wbuf, wobuf, stage, kvbuf, qbuf, top, mix, ltop, lmix, ostage, lstage, orecv, lrecv, obuf, y, raw, wave,
            wsem, xsem, ssem, rsem, kvsem, qsem, ossem, orsem, lssem, lrsem):
    own, d = a.shape
    me = lax.axis_index("sp")
    low, shift = lax.div(me, 4) == 0, lax.rem(me, 4) * 8
    e = HEAD**-0.5 * LOG2E
    to = lambda p: {"sp": p}
    bit = lambda mask, b: (lax.shift_right_logical(mask, b) & 1) == 1

    def count(mask):
        return sum(lax.shift_right_logical(mask, jnp.int32(b)) & 1 for b in range(n))

    def kind(u):
        return _choose(u, ORDER)

    def look(table, c):
        out = jnp.int32(0)
        for i, row in enumerate(table):
            half = [_signed(sum(v << 8 * b for b, v in enumerate(row[at : at + 4]))) for at in (0, 4)]
            out = jnp.where(c == i, jnp.where(low, half[0], half[1]), out)
        return lax.shift_right_logical(out, shift) & 255

    def await_many(ref, sem, number, most):
        for k in range(1, most + 1):
            @pl.when(number == k)
            def _():
                pltpu.make_async_copy(ref.at[pl.ds(0, k)], ref.at[pl.ds(0, k)], sem).wait()

    blocks = xsem.shape[0]
    some = own // blocks

    def getx(b):
        return pltpu.make_async_copy(x_hbm.at[pl.ds(b * some, some)], a.at[pl.ds(b * some, some)], xsem.at[b])

    getx(0).start()
    barrier = pltpu.get_barrier_semaphore()
    for k in range(1, n):
        pl.semaphore_signal(barrier, inc=1, device_id=to(lax.rem(me + k, n)), device_id_type=MESH)

    def load(u, k):
        @pl.when(u < units)
        def _():
            cols = pl.ds(pl.multiple_of(u * TILE, TILE), TILE)
            pltpu.make_async_copy((wk, wv, wq)[k].at[:, cols], wbuf.at[k], wsem.at[k]).start()

    def load_out(u):
        rows = pl.ds(pl.multiple_of(u * TILE, TILE), TILE)
        return pltpu.make_async_copy(wo.at[rows, :], wobuf.at[lax.rem(u, 2)], wsem.at[3 + lax.rem(u, 2)])

    load(jnp.int32(0), 0)
    for b in range(1, blocks):
        getx(b).start()
    for k in (1, 2):
        load(jnp.int32(0), k)
    cos, sin = cos_ref[...], sin_ref[...]
    wave[0, 0], wave[0, 1] = jnp.concatenate([cos, cos], axis=1), jnp.concatenate([-sin, sin], axis=1)
    wave[1, 0], wave[1, 1] = jnp.ones((own, HEAD), jnp.float32), jnp.zeros((own, HEAD), jnp.float32)
    raw[...] = jnp.zeros_like(raw)
    gain = jnp.concatenate([gain_ref[i : i + 1, :].astype(jnp.float32) for i in range(d // HEAD)], axis=1)
    chunk = 16

    def norm(i, _):
        rows = pl.ds(pl.multiple_of(i * chunk, chunk), chunk)
        values = a[rows, :].astype(jnp.float32)
        scale = lax.rsqrt(jnp.mean(values * values, -1, keepdims=True) + 1e-6)
        a[rows, :] = (values * scale * gain).astype(jnp.bfloat16)
        return 0

    for b in range(blocks):
        getx(b).wait()
        lax.fori_loop(b * some // chunk, (b + 1) * some // chunk, norm, 0)
    pl.semaphore_wait(barrier, n - 1)

    def send_kv(u):
        mask = look(plan.kv_to, kind(u))
        for p in range(n):
            @pl.when(bit(mask, p))
            def _():
                pltpu.make_async_remote_copy(
                    src_ref=stage.at[u, pl.ds(0, 2)], dst_ref=kvrecv.at[u, me], send_sem=ssem.at[u], recv_sem=rsem.at[u],
                    device_id=to(p), device_id_type=MESH).start()

    def send_q(u):
        mask = look(plan.q_to, kind(u))
        for p in range(n):
            @pl.when(bit(mask, p))
            def _():
                pltpu.make_async_remote_copy(
                    src_ref=stage.at[u, 2], dst_ref=qrecv.at[u, me], send_sem=ssem.at[u], recv_sem=rsem.at[u],
                    device_id=to(p), device_id_type=MESH).start()

    def keep(t):
        u, k = lax.div(t, 3), lax.rem(t, 3)
        spin = jnp.where(k == 1, 1, 0)
        for h in range(TWO):
            f = raw[lax.rem(t, 2), :, h * HEAD : (h + 1) * HEAD].astype(jnp.bfloat16).astype(jnp.float32)
            stage[u, k, h] = (f * wave[spin, 0] + pltpu.roll(f, HEAD // 2, 1) * wave[spin, 1]).astype(jnp.bfloat16)

    def across(u):
        for h in range(TWO):
            turned = stage[u, 1, h].T
            stage[u, 1, h, :HEAD] = turned[:, :HEAD]
            stage[u, 1, h, HEAD:] = turned[:, HEAD:]

    def multiply(k, it):
        t = 3 * it + k
        pltpu.make_async_copy(wbuf.at[k], wbuf.at[k], wsem.at[k]).wait()
        raw[lax.rem(t, 2)] = _dot(a[...], wbuf[k], 1, 0)
        keep(jnp.maximum(t - 1, 0))

        @pl.when(it + 1 < units)
        def _():
            cols = pl.ds(pl.multiple_of((it + 1) * TILE, TILE), TILE)
            for i, w in enumerate((wk, wv, wq)):
                @pl.when(k == i)
                def _():
                    pltpu.make_async_copy(w.at[:, cols], wbuf.at[k], wsem.at[k]).start()

        return it

    def fetch(u):
        c, slot = kind(u), lax.rem(u, 2)
        kvs, qs = look(plan.kv_from, c), look(plan.q_from, c)
        await_many(stage.at[:, 0], rsem.at[u], 2 * count(kvs) + count(qs), 3 * (n - 1))
        for p in range(n):
            @pl.when(bit(kvs, p))
            def _():
                pltpu.make_async_copy(kvrecv.at[u, p], kvbuf.at[slot, p], kvsem.at[slot, p]).start()

            @pl.when(bit(qs, p))
            def _():
                pltpu.make_async_copy(qrecv.at[u, p], qbuf.at[slot, p], qsem.at[slot, p]).start()

    def attend(u):
        c, slot, kept, start = kind(u), lax.rem(u, 2), lax.rem(u, KEPT), look(plan.start, u)
        kvs, qs = look(plan.kv_from, c), look(plan.q_from, c)
        masks = [look([kinds[j] for kinds in plan.jobs], c) for j in range(n)]
        places = [look(table, c) for table in plan.place]
        number = count(qs)

        kvbuf[slot, me] = stage[u, pl.ds(0, 2)]
        qbuf[slot, me] = stage[u, 2]
        for p in range(n):
            @pl.when(bit(kvs, p))
            def _():
                pltpu.make_async_copy(kvrecv.at[u, p], kvbuf.at[slot, p], kvsem.at[slot, p]).wait()

            @pl.when(bit(qs, p))
            def _():
                pltpu.make_async_copy(qrecv.at[u, p], qbuf.at[slot, p], qsem.at[slot, p]).wait()

        ones = jnp.ones((8, own), jnp.bfloat16)

        def lowest(mask):
            return _first([(lax.shift_right_logical(mask, jnp.int32(b)) & 1) == 1 for b in range(n)])

        def block(some, j, diagonal=False):
            scores, weights, keeps = [], [], []
            for h in range(TWO):
                keys = [kvbuf[slot, i, 0, h] for i in some]
                scores.append(_dot(jnp.concatenate(keys, axis=0) if len(some) > 1 else keys[0], qbuf[slot, j, h], 1, 1))
            for h, s in enumerate(scores):
                if diagonal:
                    seen = lax.broadcasted_iota(jnp.int32, s.shape, 1) >= lax.broadcasted_iota(jnp.int32, s.shape, 0)
                    s = jnp.where(seen, s, NEG)
                old = top[h]
                best = jnp.maximum(old, s.max(axis=0, keepdims=True))
                top[h] = best
                weights.append(jnp.exp2((s - best) * e).astype(jnp.bfloat16))
                keeps.append(jnp.exp2((old - best) * e))
            for h in range(TWO):
                values = []
                for i in some:
                    v = kvbuf[slot, i, 1, h]
                    values += [v[:HEAD], v[HEAD:]]
                values = jnp.concatenate([jnp.concatenate(values, axis=1)] + [jnp.concatenate([ones] * len(some), axis=1)], axis=0)
                mix[h] = mix[h] * keeps[h] + _dot(values, weights[h], 1, 0)

        def mine(j):
            return start + count(qs & ((1 << j) - 1))

        def send_back(j):
            place = sum((lax.shift_right_logical(m, j) & 1) << b for b, m in enumerate(places))
            pltpu.make_async_remote_copy(
                src_ref=ostage.at[mine(j)], dst_ref=orecv.at[u, place], send_sem=ossem.at[u], recv_sem=orsem.at[u],
                device_id=to(j), device_id_type=MESH).start()
            pltpu.make_async_remote_copy(
                src_ref=lstage.at[mine(j)], dst_ref=lrecv.at[u, place], send_sem=lssem.at[u], recv_sem=lrsem.at[u],
                device_id=to(j), device_id_type=MESH).start()

        def meet(j, mask):
            many = count(mask)

            def pair(_, mask):
                rest = mask & (mask - 1)
                block([lowest(mask), lowest(rest)], j)
                return rest & (rest - 1)

            mask = lax.fori_loop(0, lax.div(many, 2), pair, mask)

            @pl.when(lax.rem(many, 2) == 1)
            def _():
                block([lowest(mask)], j)

        def clear():
            top[...] = jnp.full_like(top, NEG)
            mix[...] = jnp.zeros_like(mix)

        def job(_, state):
            left, last = state
            j = lowest(left)
            clear()
            meet(j, _choose(j, masks))

            @pl.when(last >= 0)
            def _():
                send_back(last)

            slot = mine(j)
            for h in range(TWO):
                total = mix[h, HEAD : HEAD + 1, :]
                ostage[slot, h] = (mix[h, :HEAD, :] * (1 / total)).astype(jnp.bfloat16)
                lstage[slot, h : h + 1, :] = top[h] * e + jnp.log(total) * LOG2E
            return left & (left - 1), j

        _, last = lax.fori_loop(0, number, job, (qs, jnp.int32(-1)))
        clear()
        block([me], me, True)

        @pl.when(last >= 0)
        def _():
            send_back(last)

        meet(me, _choose(me, masks) & ~(1 << me))
        ltop[kept] = top[...]
        lmix[kept] = mix[...]

    def sent(u):
        c = kind(u)
        away = count(look(plan.q_from, c))
        await_many(stage.at[:, 0], ssem.at[u], 2 * count(look(plan.kv_to, c)) + count(look(plan.q_to, c)), 3 * (n - 1))
        await_many(ostage, ossem.at[u], away, n - 1)
        await_many(lstage, lssem.at[u], away, n - 1)

    def finish(u):
        c, kept = kind(u), lax.rem(u, KEPT)
        number = count(look(plan.q_to, c))
        await_many(orecv.at[u], orsem.at[u], number, plan.most)
        await_many(lrecv.at[u], lrsem.at[u], number, plan.most)
        for parts in range(plan.most + 1):
            @pl.when(number == parts)
            def _():
                for h in range(TWO):
                    base = ltop[kept, h] * e
                    logs = [lrecv[u, r, h : h + 1, :] for r in range(parts)]
                    best = functools.reduce(jnp.maximum, logs, base)
                    keep = jnp.exp2(base - best)
                    total = lmix[kept, h, HEAD : HEAD + 1, :] * keep
                    out = lmix[kept, h, :HEAD, :] * keep
                    for r in range(parts):
                        w = jnp.exp2(logs[r] - best)
                        total += w
                        out += orecv[u, r, h].astype(jnp.float32) * w
                    obuf[:, h * HEAD : (h + 1) * HEAD] = (out * (1 / total)).T.astype(jnp.bfloat16)

        load_out(u).wait()
        slot = lax.rem(u, 2)

        @pl.when(u == 0)
        def _():
            for at in range(0, d, TILE):
                y[:, at : at + TILE] = _dot(obuf[...], wobuf[slot, :, at : at + TILE], 1, 0)

        @pl.when((u > 0) & (u < units - 1))
        def _():
            for at in range(0, d, TILE):
                y[:, at : at + TILE] += _dot(obuf[...], wobuf[slot, :, at : at + TILE], 1, 0)

        @pl.when(u == units - 1)
        def _():
            for b in range(blocks):
                getx(b).wait()
            for at in range(0, d, TILE):
                got = y[:, at : at + TILE] + _dot(obuf[...], wobuf[slot, :, at : at + TILE], 1, 0)
                a[:, at : at + TILE] = (a[:, at : at + TILE].astype(jnp.float32) + got).astype(jnp.bfloat16)

    def step(it, _):
        @pl.when((it >= BACK - 1) & (it < units + BACK - 1))
        def _():
            load_out(it - (BACK - 1)).start()

        @pl.when(it < units)
        def _():
            lax.fori_loop(0, 3, multiply, it)
            across(it)

        @pl.when(it == units)
        def _():
            keep(3 * it - 1)

        @pl.when((it > 0) & (it <= units))
        def _():
            send_q(it - 1)

        @pl.when(it == units)
        def _():
            for b in range(blocks):
                getx(b).start()

        @pl.when(it < units)
        def _():
            send_kv(it)

        @pl.when((it >= LAG) & (it < units + LAG))
        def _():
            attend(it - LAG)

        @pl.when(it >= BACK)
        def _():
            finish(it - BACK)

        @pl.when(it >= BACK + LATE)
        def _():
            sent(it - (BACK + LATE))

        @pl.when((it >= LAG - 1) & (it < units + LAG - 1))
        def _():
            fetch(it - (LAG - 1))

        return 0

    lax.fori_loop(0, units + BACK, step, 0)

    for u in range(units - LATE, units):
        sent(jnp.int32(u))


def solution(mesh):
    n = mesh.shape["sp"]

    def step(x, gain, wq, wk, wv, wo):
        own, d = x.shape
        units = wq.shape[1] // TILE
        plan = Plan(n)
        half = HEAD // 2
        place = lax.axis_index("sp") * own + jnp.arange(own)
        angle = place.astype(jnp.float32)[:, None] * THETA ** (-jnp.arange(half, dtype=jnp.float32) / half)
        cos, sin = jnp.cos(angle), jnp.sin(angle)
        blocks = 4
        hbm, vmem = pl.BlockSpec(memory_space=pl.ANY), pl.BlockSpec(memory_space=pltpu.VMEM)
        bf16, f32 = jnp.bfloat16, jnp.float32
        dma = pltpu.SemaphoreType.DMA
        return pl.pallas_call(
            functools.partial(_kernel, n, units, plan),
            name="layer",
            out_shape=[
                pltpu.VMEM((own, d), bf16),
                jax.ShapeDtypeStruct((units, n, 2, TWO, own, HEAD), bf16),
                jax.ShapeDtypeStruct((units, n, TWO, own, HEAD), bf16),
            ],
            in_specs=[hbm, vmem, vmem, vmem, hbm, hbm, hbm, hbm],
            out_specs=[vmem, hbm, hbm],
            scratch_shapes=[
                pltpu.VMEM((3, d, TILE), bf16),
                pltpu.VMEM((2, TILE, d), bf16),
                pltpu.VMEM((units, 3, TWO, own, HEAD), bf16),
                pltpu.VMEM((2, n, 2, TWO, own, HEAD), bf16),
                pltpu.VMEM((2, n, TWO, own, HEAD), bf16),
                pltpu.VMEM((TWO, 1, own), f32),
                pltpu.VMEM((TWO, HEAD + 8, own), f32),
                pltpu.VMEM((KEPT, TWO, 1, own), f32),
                pltpu.VMEM((KEPT, TWO, HEAD + 8, own), f32),
                pltpu.VMEM((plan.held, TWO, HEAD, own), bf16),
                pltpu.VMEM((plan.held, TWO, own), f32),
                pltpu.VMEM((units, plan.most, TWO, HEAD, own), bf16),
                pltpu.VMEM((units, plan.most, TWO, own), f32),
                pltpu.VMEM((own, TILE), bf16),
                pltpu.VMEM((own, d), f32),
                pltpu.VMEM((2, own, TILE), f32),
                pltpu.VMEM((2, 2, own, HEAD), f32),
                dma((5,)), dma((blocks,)), dma((units,)), dma((units,)), dma((2, n)), dma((2, n)),
                dma((units,)), dma((units,)), dma((units,)), dma((units,)),
            ],
            compiler_params=pltpu.CompilerParams(collective_id=0, has_side_effects=True, vmem_limit_bytes=63000000),
        )(x, gain.reshape(d // HEAD, HEAD), cos, sin, wq, wk, wv, wo)[0]

    tokens, whole = P(("dp", "sp"), None), P(None, None)
    return jax.shard_map(
        step,
        mesh=mesh,
        in_specs=(tokens, P(None), whole, whole, whole, whole),
        out_specs=tokens,
        check_vma=False,
    )
```

```python
import functools

import jax
import jax.numpy as jnp
from jax import lax
from jax.experimental import pallas as pl
from jax.experimental.pallas import tpu as pltpu
from jax.sharding import PartitionSpec as P

HEAD = 128
THETA = 10000
TWO = 2
TILE = TWO * HEAD
LAG = 6
BACK = 11
KEPT = BACK - LAG + 1
LATE = 6
LOG2E = 1.4426950408889634
NEG = -1e30
MESH = pl.DeviceIdType.MESH

PLACES = (
    (0o40004222222221, 0o4440004440004),
    (0o22222222222220, 0o66222226222222),
    (0o44664466466111, 0o66444666444664),
    (0o11111111111111, 0o66111116111111),
    (0o33333333333330, 0o77333336333333),
    (0o47774777777111, 0o74447774447774),
    (0o33333333333330, 0o66333336333333),
    (0o3222222220, 0o55500005500005),
    (0o55555555555111, 0o75555555555555),
    (0o33333333333330, 0o73333333333333),
    (0o40004222222220, 0o4440004440004),
    (0o55555555555111, 0o55555555555555),
    (0o2222222220, 0o0),
    (0o44774477411111, 0o74444774444774),
)
ORDER = (0, 6, 3, 8, 10, 5, 1, 6, 8, 3, 4, 5, 1, 7, 2, 6, 3, 5, 1, 11, 6, 13, 12, 3, 11, 9, 1, 5)


class Plan:
    def __init__(self, n):
        self.jobs = []
        for first, second in PLACES:
            code = first + (second << 42)
            jobs = [[1 << j if j == d else 0 for d in range(n)] for j in range(n)]
            for j in range(1, n):
                for i in range(j):
                    jobs[j][code % 8] |= 1 << i
                    code //= 8
            self.jobs.append(jobs)
        kinds, devs = range(len(PLACES)), range(n)
        bits = lambda test: sum(1 << x for x in devs if test(x))
        need = lambda c, d, i: i != d and any(self.jobs[c][j][d] >> i & 1 for j in devs)
        away = lambda c, d, j: j != d and self.jobs[c][j][d] != 0
        self.kv_to = [[bits(lambda d: need(c, d, i)) for i in devs] for c in kinds]
        self.kv_from = [[bits(lambda i: need(c, d, i)) for d in devs] for c in kinds]
        self.q_to = [[bits(lambda d: away(c, d, j)) for j in devs] for c in kinds]
        self.q_from = [[bits(lambda j: away(c, d, j)) for d in devs] for c in kinds]
        self.most = max(bin(b).count("1") for row in self.q_to for b in row)
        rank = lambda c, d, j: bin(self.q_to[c][j] & ((1 << d) - 1)).count("1")
        held = [[bin(self.q_from[ORDER[u]][d]).count("1") for d in devs] for u in range(len(ORDER))]
        self.start = [[sum(row[d] for row in held[:u]) for d in devs] for u in range(len(ORDER))]
        self.held = max(sum(row[d] for row in held) for d in devs)
        self.place = [[[bits(lambda j: away(c, d, j) and rank(c, d, j) >> b & 1) for d in devs] for c in kinds] for b in range(2)]


def _dot(a, b, ca, cb):
    return lax.dot_general(a, b, (((ca,), (cb,)), ((), ())), preferred_element_type=jnp.float32)


def _choose(index, values):
    out = jnp.int32(values[0])
    for i, v in enumerate(values[1:], 1):
        out = jnp.where(index == i, v, out)
    return out


def _first(tests):
    out = jnp.int32(0)
    for i in range(len(tests) - 1, -1, -1):
        out = jnp.where(tests[i], i, out)
    return out


def _signed(x):
    return jnp.int32(x - (1 << 32) if x >> 31 else x)


def _kernel(n, units, plan, x_hbm, gain_ref, cos_ref, sin_ref, wq, wk, wv, wo, a, kvrecv, qrecv,
            wbuf, wobuf, stage, kvbuf, qbuf, top, mix, ltop, lmix, ostage, lstage, orecv, lrecv, obuf, y, raw, wave,
            wsem, xsem, ssem, rsem, kvsem, qsem, ossem, orsem, lssem, lrsem):
    own, d = a.shape
    me = lax.axis_index("sp")
    low, shift = lax.div(me, 4) == 0, lax.rem(me, 4) * 8
    e = HEAD**-0.5 * LOG2E
    to = lambda p: {"sp": p}
    bit = lambda mask, b: (lax.shift_right_logical(mask, b) & 1) == 1

    def count(mask):
        return sum(lax.shift_right_logical(mask, jnp.int32(b)) & 1 for b in range(n))

    def kind(u):
        return _choose(u, ORDER)

    def look(table, c):
        out = jnp.int32(0)
        for i, row in enumerate(table):
            half = [_signed(sum(v << 8 * b for b, v in enumerate(row[at : at + 4]))) for at in (0, 4)]
            out = jnp.where(c == i, jnp.where(low, half[0], half[1]), out)
        return lax.shift_right_logical(out, shift) & 255

    def await_many(ref, sem, number, most):
        for k in range(1, most + 1):
            @pl.when(number == k)
            def _():
                pltpu.make_async_copy(ref.at[pl.ds(0, k)], ref.at[pl.ds(0, k)], sem).wait()

    blocks = xsem.shape[0]
    some = own // blocks

    def getx(b):
        return pltpu.make_async_copy(x_hbm.at[pl.ds(b * some, some)], a.at[pl.ds(b * some, some)], xsem.at[b])

    getx(0).start()
    barrier = pltpu.get_barrier_semaphore()
    for k in range(1, n):
        pl.semaphore_signal(barrier, inc=1, device_id=to(lax.rem(me + k, n)), device_id_type=MESH)

    def load(u, k):
        @pl.when(u < units)
        def _():
            cols = pl.ds(pl.multiple_of(u * TILE, TILE), TILE)
            pltpu.make_async_copy((wk, wv, wq)[k].at[:, cols], wbuf.at[k], wsem.at[k]).start()

    def load_out(u):
        rows = pl.ds(pl.multiple_of(u * TILE, TILE), TILE)
        return pltpu.make_async_copy(wo.at[rows, :], wobuf.at[lax.rem(u, 2)], wsem.at[3 + lax.rem(u, 2)])

    load(jnp.int32(0), 0)
    for b in range(1, blocks):
        getx(b).start()
    for k in (1, 2):
        load(jnp.int32(0), k)
    cos, sin = cos_ref[...], sin_ref[...]
    wave[0, 0], wave[0, 1] = jnp.concatenate([cos, cos], axis=1), jnp.concatenate([-sin, sin], axis=1)
    wave[1, 0], wave[1, 1] = jnp.ones((own, HEAD), jnp.float32), jnp.zeros((own, HEAD), jnp.float32)
    raw[...] = jnp.zeros_like(raw)
    gain = jnp.concatenate([gain_ref[i : i + 1, :].astype(jnp.float32) for i in range(d // HEAD)], axis=1)
    chunk = 16

    def norm(i, _):
        rows = pl.ds(pl.multiple_of(i * chunk, chunk), chunk)
        values = a[rows, :].astype(jnp.float32)
        scale = lax.rsqrt(jnp.mean(values * values, -1, keepdims=True) + 1e-6)
        a[rows, :] = (values * scale * gain).astype(jnp.bfloat16)
        return 0

    for b in range(blocks):
        getx(b).wait()
        lax.fori_loop(b * some // chunk, (b + 1) * some // chunk, norm, 0, unroll=4)
    pl.semaphore_wait(barrier, n - 1)

    def send_kv(u):
        mask = look(plan.kv_to, kind(u))
        for p in range(n):
            @pl.when(bit(mask, p))
            def _():
                pltpu.make_async_remote_copy(
                    src_ref=stage.at[u, pl.ds(0, 2)], dst_ref=kvrecv.at[u, me], send_sem=ssem.at[u], recv_sem=rsem.at[u],
                    device_id=to(p), device_id_type=MESH).start()

    def send_q(u):
        mask = look(plan.q_to, kind(u))
        for p in range(n):
            @pl.when(bit(mask, p))
            def _():
                pltpu.make_async_remote_copy(
                    src_ref=stage.at[u, 2], dst_ref=qrecv.at[u, me], send_sem=ssem.at[u], recv_sem=rsem.at[u],
                    device_id=to(p), device_id_type=MESH).start()

    def keep(t):
        u, k = lax.div(t, 3), lax.rem(t, 3)
        spin = jnp.where(k == 1, 1, 0)
        for h in range(TWO):
            f = raw[lax.rem(t, 2), :, h * HEAD : (h + 1) * HEAD].astype(jnp.bfloat16).astype(jnp.float32)
            stage[u, k, h] = (f * wave[spin, 0] + pltpu.roll(f, HEAD // 2, 1) * wave[spin, 1]).astype(jnp.bfloat16)

    def across(u):
        for h in range(TWO):
            turned = stage[u, 1, h].T
            stage[u, 1, h, :HEAD] = turned[:, :HEAD]
            stage[u, 1, h, HEAD:] = turned[:, HEAD:]

    def multiply(k, it):
        t = 3 * it + k
        pltpu.make_async_copy(wbuf.at[k], wbuf.at[k], wsem.at[k]).wait()
        raw[lax.rem(t, 2)] = _dot(a[...], wbuf[k], 1, 0)
        keep(jnp.maximum(t - 1, 0))

        @pl.when(it + 1 < units)
        def _():
            cols = pl.ds(pl.multiple_of((it + 1) * TILE, TILE), TILE)
            for i, w in enumerate((wk, wv, wq)):
                @pl.when(k == i)
                def _():
                    pltpu.make_async_copy(w.at[:, cols], wbuf.at[k], wsem.at[k]).start()

        return it

    def fetch(u):
        c, slot = kind(u), lax.rem(u, 2)
        kvs, qs = look(plan.kv_from, c), look(plan.q_from, c)
        await_many(stage.at[:, 0], rsem.at[u], 2 * count(kvs) + count(qs), 3 * (n - 1))
        for p in range(n):
            @pl.when(bit(kvs, p))
            def _():
                pltpu.make_async_copy(kvrecv.at[u, p], kvbuf.at[slot, p], kvsem.at[slot, p]).start()

            @pl.when(bit(qs, p))
            def _():
                pltpu.make_async_copy(qrecv.at[u, p], qbuf.at[slot, p], qsem.at[slot, p]).start()

    def attend(u):
        c, slot, kept, start = kind(u), lax.rem(u, 2), lax.rem(u, KEPT), look(plan.start, u)
        kvs, qs = look(plan.kv_from, c), look(plan.q_from, c)
        masks = [look([kinds[j] for kinds in plan.jobs], c) for j in range(n)]
        places = [look(table, c) for table in plan.place]
        number = count(qs)

        kvbuf[slot, me] = stage[u, pl.ds(0, 2)]
        qbuf[slot, me] = stage[u, 2]
        for p in range(n):
            @pl.when(bit(kvs, p))
            def _():
                pltpu.make_async_copy(kvrecv.at[u, p], kvbuf.at[slot, p], kvsem.at[slot, p]).wait()

            @pl.when(bit(qs, p))
            def _():
                pltpu.make_async_copy(qrecv.at[u, p], qbuf.at[slot, p], qsem.at[slot, p]).wait()

        ones = jnp.ones((8, own), jnp.bfloat16)

        def lowest(mask):
            return _first([(lax.shift_right_logical(mask, jnp.int32(b)) & 1) == 1 for b in range(n)])

        def block(some, j, diagonal=False):
            scores, weights, keeps = [], [], []
            for h in range(TWO):
                keys = [kvbuf[slot, i, 0, h] for i in some]
                scores.append(_dot(jnp.concatenate(keys, axis=0) if len(some) > 1 else keys[0], qbuf[slot, j, h], 1, 1))
            for h, s in enumerate(scores):
                if diagonal:
                    seen = lax.broadcasted_iota(jnp.int32, s.shape, 1) >= lax.broadcasted_iota(jnp.int32, s.shape, 0)
                    s = jnp.where(seen, s, NEG)
                old = top[h]
                best = jnp.maximum(old, s.max(axis=0, keepdims=True))
                top[h] = best
                weights.append(jnp.exp2((s - best) * e).astype(jnp.bfloat16))
                keeps.append(jnp.exp2((old - best) * e))
            for h in range(TWO):
                values = []
                for i in some:
                    v = kvbuf[slot, i, 1, h]
                    values += [v[:HEAD], v[HEAD:]]
                values = jnp.concatenate([jnp.concatenate(values, axis=1)] + [jnp.concatenate([ones] * len(some), axis=1)], axis=0)
                mix[h] = mix[h] * keeps[h] + _dot(values, weights[h], 1, 0)

        def mine(j):
            return start + count(qs & ((1 << j) - 1))

        def send_back(j):
            place = sum((lax.shift_right_logical(m, j) & 1) << b for b, m in enumerate(places))
            pltpu.make_async_remote_copy(
                src_ref=ostage.at[mine(j)], dst_ref=orecv.at[u, place], send_sem=ossem.at[u], recv_sem=orsem.at[u],
                device_id=to(j), device_id_type=MESH).start()
            pltpu.make_async_remote_copy(
                src_ref=lstage.at[mine(j)], dst_ref=lrecv.at[u, place], send_sem=lssem.at[u], recv_sem=lrsem.at[u],
                device_id=to(j), device_id_type=MESH).start()

        def meet(j, mask):
            many = count(mask)

            def several(number):
                def go(_, mask):
                    some = []
                    for _ in range(number):
                        some.append(lowest(mask))
                        mask = mask & (mask - 1)
                    block(some, j)
                    return mask

                return go

            mask = lax.fori_loop(0, lax.div(many, 4), several(4), mask)
            mask = lax.fori_loop(0, lax.div(lax.rem(many, 4), 2), several(2), mask)

            @pl.when(lax.rem(many, 2) == 1)
            def _():
                block([lowest(mask)], j)

        def clear():
            top[...] = jnp.full_like(top, NEG)
            mix[...] = jnp.zeros_like(mix)

        def job(_, state):
            left, last = state
            j = lowest(left)
            clear()
            meet(j, _choose(j, masks))

            @pl.when(last >= 0)
            def _():
                send_back(last)

            slot = mine(j)
            for h in range(TWO):
                total = mix[h, HEAD : HEAD + 1, :]
                ostage[slot, h] = (mix[h, :HEAD, :] * (1 / total)).astype(jnp.bfloat16)
                lstage[slot, h : h + 1, :] = top[h] * e + jnp.log(total) * LOG2E
            return left & (left - 1), j

        _, last = lax.fori_loop(0, number, job, (qs, jnp.int32(-1)))
        clear()
        block([me], me, True)

        @pl.when(last >= 0)
        def _():
            send_back(last)

        meet(me, _choose(me, masks) & ~(1 << me))
        ltop[kept] = top[...]
        lmix[kept] = mix[...]

    def sent(u):
        c = kind(u)
        away = count(look(plan.q_from, c))
        await_many(stage.at[:, 0], ssem.at[u], 2 * count(look(plan.kv_to, c)) + count(look(plan.q_to, c)), 3 * (n - 1))
        await_many(ostage, ossem.at[u], away, n - 1)
        await_many(lstage, lssem.at[u], away, n - 1)

    def finish(u):
        c, kept = kind(u), lax.rem(u, KEPT)
        number = count(look(plan.q_to, c))
        await_many(orecv.at[u], orsem.at[u], number, plan.most)
        await_many(lrecv.at[u], lrsem.at[u], number, plan.most)
        for parts in range(plan.most + 1):
            @pl.when(number == parts)
            def _():
                for h in range(TWO):
                    base = ltop[kept, h] * e
                    logs = [lrecv[u, r, h : h + 1, :] for r in range(parts)]
                    best = functools.reduce(jnp.maximum, logs, base)
                    keep = jnp.exp2(base - best)
                    total = lmix[kept, h, HEAD : HEAD + 1, :] * keep
                    out = lmix[kept, h, :HEAD, :] * keep
                    for r in range(parts):
                        w = jnp.exp2(logs[r] - best)
                        total += w
                        out += orecv[u, r, h].astype(jnp.float32) * w
                    obuf[:, h * HEAD : (h + 1) * HEAD] = (out * (1 / total)).T.astype(jnp.bfloat16)

        load_out(u).wait()
        slot = lax.rem(u, 2)

        @pl.when(u == 0)
        def _():
            for at in range(0, d, TILE):
                y[:, at : at + TILE] = _dot(obuf[...], wobuf[slot, :, at : at + TILE], 1, 0)

        @pl.when((u > 0) & (u < units - 1))
        def _():
            for at in range(0, d, TILE):
                y[:, at : at + TILE] += _dot(obuf[...], wobuf[slot, :, at : at + TILE], 1, 0)

        @pl.when(u == units - 1)
        def _():
            for b in range(blocks):
                getx(b).wait()
            for at in range(0, d, TILE):
                got = y[:, at : at + TILE] + _dot(obuf[...], wobuf[slot, :, at : at + TILE], 1, 0)
                a[:, at : at + TILE] = (a[:, at : at + TILE].astype(jnp.float32) + got).astype(jnp.bfloat16)

    def step(it, _):
        @pl.when((it >= BACK - 1) & (it < units + BACK - 1))
        def _():
            load_out(it - (BACK - 1)).start()

        @pl.when(it < units)
        def _():
            lax.fori_loop(0, 3, multiply, it)
            across(it)

        @pl.when(it == units)
        def _():
            keep(3 * it - 1)

        @pl.when((it > 0) & (it <= units))
        def _():
            send_q(it - 1)

        @pl.when(it == units)
        def _():
            for b in range(blocks):
                getx(b).start()

        @pl.when(it < units)
        def _():
            send_kv(it)

        @pl.when((it >= LAG) & (it < units + LAG))
        def _():
            attend(it - LAG)

        @pl.when(it >= BACK)
        def _():
            finish(it - BACK)

        @pl.when(it >= BACK + LATE)
        def _():
            sent(it - (BACK + LATE))

        @pl.when((it >= LAG - 1) & (it < units + LAG - 1))
        def _():
            fetch(it - (LAG - 1))

        return 0

    lax.fori_loop(0, units + BACK, step, 0)

    for u in range(units - LATE, units):
        sent(jnp.int32(u))


def solution(mesh):
    n = mesh.shape["sp"]

    def step(x, gain, wq, wk, wv, wo):
        own, d = x.shape
        units = wq.shape[1] // TILE
        plan = Plan(n)
        half = HEAD // 2
        place = lax.axis_index("sp") * own + jnp.arange(own)
        angle = place.astype(jnp.float32)[:, None] * THETA ** (-jnp.arange(half, dtype=jnp.float32) / half)
        cos, sin = jnp.cos(angle), jnp.sin(angle)
        blocks = 4
        hbm, vmem = pl.BlockSpec(memory_space=pl.ANY), pl.BlockSpec(memory_space=pltpu.VMEM)
        bf16, f32 = jnp.bfloat16, jnp.float32
        dma = pltpu.SemaphoreType.DMA
        return pl.pallas_call(
            functools.partial(_kernel, n, units, plan),
            name="layer",
            out_shape=[
                pltpu.VMEM((own, d), bf16),
                jax.ShapeDtypeStruct((units, n, 2, TWO, own, HEAD), bf16),
                jax.ShapeDtypeStruct((units, n, TWO, own, HEAD), bf16),
            ],
            in_specs=[hbm, vmem, vmem, vmem, hbm, hbm, hbm, hbm],
            out_specs=[vmem, hbm, hbm],
            scratch_shapes=[
                pltpu.VMEM((3, d, TILE), bf16),
                pltpu.VMEM((2, TILE, d), bf16),
                pltpu.VMEM((units, 3, TWO, own, HEAD), bf16),
                pltpu.VMEM((2, n, 2, TWO, own, HEAD), bf16),
                pltpu.VMEM((2, n, TWO, own, HEAD), bf16),
                pltpu.VMEM((TWO, 1, own), f32),
                pltpu.VMEM((TWO, HEAD + 8, own), f32),
                pltpu.VMEM((KEPT, TWO, 1, own), f32),
                pltpu.VMEM((KEPT, TWO, HEAD + 8, own), f32),
                pltpu.VMEM((plan.held, TWO, HEAD, own), bf16),
                pltpu.VMEM((plan.held, TWO, own), f32),
                pltpu.VMEM((units, plan.most, TWO, HEAD, own), bf16),
                pltpu.VMEM((units, plan.most, TWO, own), f32),
                pltpu.VMEM((own, TILE), bf16),
                pltpu.VMEM((own, d), f32),
                pltpu.VMEM((2, own, TILE), f32),
                pltpu.VMEM((2, 2, own, HEAD), f32),
                dma((5,)), dma((blocks,)), dma((units,)), dma((units,)), dma((2, n)), dma((2, n)),
                dma((units,)), dma((units,)), dma((units,)), dma((units,)),
            ],
            compiler_params=pltpu.CompilerParams(collective_id=0, has_side_effects=True, vmem_limit_bytes=63300000),
        )(x, gain.reshape(d // HEAD, HEAD), cos, sin, wq, wk, wv, wo)[0]

    tokens, whole = P(("dp", "sp"), None), P(None, None)
    return jax.shard_map(
        step,
        mesh=mesh,
        in_specs=(tokens, P(None), whole, whole, whole, whole),
        out_specs=tokens,
        check_vma=False,
    )
```

```python
import functools

import jax
import jax.numpy as jnp
from jax import lax
from jax.experimental import pallas as pl
from jax.experimental.pallas import tpu as pltpu
from jax.sharding import PartitionSpec as P

HEAD = 128
THETA = 10000
TWO = 2
TILE = TWO * HEAD
LAG = 6
BACK = 11
KEPT = BACK - LAG + 1
LATE = 6
LOG2E = 1.4426950408889634
NEG = -1e30
MESH = pl.DeviceIdType.MESH

PLACES = (
    (0o40004222222221, 0o4440004440004),
    (0o22222222222220, 0o66222226222222),
    (0o44664466466111, 0o66444666444664),
    (0o11111111111111, 0o66111116111111),
    (0o33333333333330, 0o77333336333333),
    (0o47774777777111, 0o74447774447774),
    (0o33333333333330, 0o66333336333333),
    (0o3222222220, 0o55500005500005),
    (0o55555555555111, 0o75555555555555),
    (0o33333333333330, 0o73333333333333),
    (0o40004222222220, 0o4440004440004),
    (0o55555555555111, 0o55555555555555),
    (0o2222222220, 0o0),
    (0o44774477411111, 0o74444774444774),
)
ORDER = (0, 6, 3, 8, 10, 5, 1, 6, 8, 3, 4, 5, 1, 7, 2, 6, 3, 5, 1, 11, 6, 13, 12, 3, 11, 9, 1, 5)


class Plan:
    def __init__(self, n):
        self.jobs = []
        for first, second in PLACES:
            code = first + (second << 42)
            jobs = [[1 << j if j == d else 0 for d in range(n)] for j in range(n)]
            for j in range(1, n):
                for i in range(j):
                    jobs[j][code % 8] |= 1 << i
                    code //= 8
            self.jobs.append(jobs)
        kinds, devs = range(len(PLACES)), range(n)
        bits = lambda test: sum(1 << x for x in devs if test(x))
        need = lambda c, d, i: i != d and any(self.jobs[c][j][d] >> i & 1 for j in devs)
        away = lambda c, d, j: j != d and self.jobs[c][j][d] != 0
        self.kv_to = [[bits(lambda d: need(c, d, i)) for i in devs] for c in kinds]
        self.kv_from = [[bits(lambda i: need(c, d, i)) for d in devs] for c in kinds]
        self.q_to = [[bits(lambda d: away(c, d, j)) for j in devs] for c in kinds]
        self.q_from = [[bits(lambda j: away(c, d, j)) for d in devs] for c in kinds]
        self.most = max(bin(b).count("1") for row in self.q_to for b in row)
        rank = lambda c, d, j: bin(self.q_to[c][j] & ((1 << d) - 1)).count("1")
        held = [[bin(self.q_from[ORDER[u]][d]).count("1") for d in devs] for u in range(len(ORDER))]
        self.start = [[sum(row[d] for row in held[:u]) for d in devs] for u in range(len(ORDER))]
        self.held = max(sum(row[d] for row in held) for d in devs)
        self.place = [[[bits(lambda j: away(c, d, j) and rank(c, d, j) >> b & 1) for d in devs] for c in kinds] for b in range(2)]


def _dot(a, b, ca, cb):
    return lax.dot_general(a, b, (((ca,), (cb,)), ((), ())), preferred_element_type=jnp.float32)


def _choose(index, values):
    out = jnp.int32(values[0])
    for i, v in enumerate(values[1:], 1):
        out = jnp.where(index == i, v, out)
    return out


def _first(tests):
    out = jnp.int32(0)
    for i in range(len(tests) - 1, -1, -1):
        out = jnp.where(tests[i], i, out)
    return out


def _signed(x):
    return jnp.int32(x - (1 << 32) if x >> 31 else x)


def _kernel(n, units, plan, x_hbm, gain_ref, cos_ref, sin_ref, wq, wk, wv, wo, a, kvrecv, qrecv,
            wbuf, wobuf, stage, kvbuf, qbuf, top, mix, ltop, lmix, ostage, lstage, orecv, lrecv, obuf, y, raw, wave,
            wsem, xsem, ssem, rsem, kvsem, qsem, ossem, orsem, lssem, lrsem):
    own, d = a.shape
    me = lax.axis_index("sp")
    low, shift = lax.div(me, 4) == 0, lax.rem(me, 4) * 8
    e = HEAD**-0.5 * LOG2E
    to = lambda p: {"sp": p}
    bit = lambda mask, b: (lax.shift_right_logical(mask, b) & 1) == 1

    def count(mask):
        return sum(lax.shift_right_logical(mask, jnp.int32(b)) & 1 for b in range(n))

    def kind(u):
        return _choose(u, ORDER)

    def look(table, c):
        out = jnp.int32(0)
        for i, row in enumerate(table):
            half = [_signed(sum(v << 8 * b for b, v in enumerate(row[at : at + 4]))) for at in (0, 4)]
            out = jnp.where(c == i, jnp.where(low, half[0], half[1]), out)
        return lax.shift_right_logical(out, shift) & 255

    def await_many(ref, sem, number, most):
        for k in range(1, most + 1):
            @pl.when(number == k)
            def _():
                pltpu.make_async_copy(ref.at[pl.ds(0, k)], ref.at[pl.ds(0, k)], sem).wait()

    blocks = xsem.shape[0]
    some = own // blocks

    def getx(b):
        return pltpu.make_async_copy(x_hbm.at[pl.ds(b * some, some)], a.at[pl.ds(b * some, some)], xsem.at[b])

    getx(0).start()
    barrier = pltpu.get_barrier_semaphore()
    for k in range(1, n):
        pl.semaphore_signal(barrier, inc=1, device_id=to(lax.rem(me + k, n)), device_id_type=MESH)

    def load(u, k):
        @pl.when(u < units)
        def _():
            cols = pl.ds(pl.multiple_of(u * TILE, TILE), TILE)
            pltpu.make_async_copy((wk, wv, wq)[k].at[:, cols], wbuf.at[k], wsem.at[k]).start()

    def load_out(u):
        rows = pl.ds(pl.multiple_of(u * TILE, TILE), TILE)
        return pltpu.make_async_copy(wo.at[rows, :], wobuf.at[lax.rem(u, 2)], wsem.at[3 + lax.rem(u, 2)])

    load(jnp.int32(0), 0)
    for b in range(1, blocks):
        getx(b).start()
    for k in (1, 2):
        load(jnp.int32(0), k)
    cos, sin = cos_ref[...], sin_ref[...]
    wave[0, 0], wave[0, 1] = jnp.concatenate([cos, cos], axis=1), jnp.concatenate([-sin, sin], axis=1)
    wave[1, 0], wave[1, 1] = jnp.ones((own, HEAD), jnp.float32), jnp.zeros((own, HEAD), jnp.float32)
    raw[...] = jnp.zeros_like(raw)
    gain = jnp.concatenate([gain_ref[i : i + 1, :].astype(jnp.float32) for i in range(d // HEAD)], axis=1)
    chunk = 16

    def norm(i, _):
        rows = pl.ds(pl.multiple_of(i * chunk, chunk), chunk)
        values = a[rows, :].astype(jnp.float32)
        scale = lax.rsqrt(jnp.mean(values * values, -1, keepdims=True) + 1e-6)
        a[rows, :] = (values * scale * gain).astype(jnp.bfloat16)
        return 0

    for b in range(blocks):
        getx(b).wait()
        lax.fori_loop(b * some // chunk, (b + 1) * some // chunk, norm, 0, unroll=4)
    pl.semaphore_wait(barrier, n - 1)

    def send_kv(u, k):
        mask = look(plan.kv_to, kind(u))
        for p in range(n):
            @pl.when(bit(mask, p))
            def _():
                pltpu.make_async_remote_copy(
                    src_ref=stage.at[u, k], dst_ref=kvrecv.at[u, me, k], send_sem=ssem.at[u], recv_sem=rsem.at[u],
                    device_id=to(p), device_id_type=MESH).start()

    def send_q(u):
        mask = look(plan.q_to, kind(u))
        for p in range(n):
            @pl.when(bit(mask, p))
            def _():
                pltpu.make_async_remote_copy(
                    src_ref=stage.at[u, 2], dst_ref=qrecv.at[u, me], send_sem=ssem.at[u], recv_sem=rsem.at[u],
                    device_id=to(p), device_id_type=MESH).start()

    def keep(t):
        u, k = lax.div(t, 3), lax.rem(t, 3)
        spin = jnp.where(k == 1, 1, 0)
        for h in range(TWO):
            f = raw[lax.rem(t, 2), :, h * HEAD : (h + 1) * HEAD].astype(jnp.bfloat16).astype(jnp.float32)
            stage[u, k, h] = (f * wave[spin, 0] + pltpu.roll(f, HEAD // 2, 1) * wave[spin, 1]).astype(jnp.bfloat16)

    def across(u):
        for h in range(TWO):
            turned = stage[u, 1, h].T
            stage[u, 1, h, :HEAD] = turned[:, :HEAD]
            stage[u, 1, h, HEAD:] = turned[:, HEAD:]

    def multiply(k, it):
        t = 3 * it + k

        @pl.when(k == 2)
        def _():
            send_kv(it, 0)

        pltpu.make_async_copy(wbuf.at[k], wbuf.at[k], wsem.at[k]).wait()
        raw[lax.rem(t, 2)] = _dot(a[...], wbuf[k], 1, 0)
        keep(jnp.maximum(t - 1, 0))

        @pl.when(it + 1 < units)
        def _():
            cols = pl.ds(pl.multiple_of((it + 1) * TILE, TILE), TILE)
            for i, w in enumerate((wk, wv, wq)):
                @pl.when(k == i)
                def _():
                    pltpu.make_async_copy(w.at[:, cols], wbuf.at[k], wsem.at[k]).start()

        return it

    def fetch(u):
        c, slot = kind(u), lax.rem(u, 2)
        kvs, qs = look(plan.kv_from, c), look(plan.q_from, c)
        await_many(stage.at[:, 0], rsem.at[u], 2 * count(kvs) + count(qs), 3 * (n - 1))
        for p in range(n):
            @pl.when(bit(kvs, p))
            def _():
                pltpu.make_async_copy(kvrecv.at[u, p], kvbuf.at[slot, p], kvsem.at[slot, p]).start()

            @pl.when(bit(qs, p))
            def _():
                pltpu.make_async_copy(qrecv.at[u, p], qbuf.at[slot, p], qsem.at[slot, p]).start()

    def attend(u):
        c, slot, kept, start = kind(u), lax.rem(u, 2), lax.rem(u, KEPT), look(plan.start, u)
        kvs, qs = look(plan.kv_from, c), look(plan.q_from, c)
        masks = [look([kinds[j] for kinds in plan.jobs], c) for j in range(n)]
        places = [look(table, c) for table in plan.place]
        number = count(qs)

        kvbuf[slot, me] = stage[u, pl.ds(0, 2)]
        qbuf[slot, me] = stage[u, 2]
        for p in range(n):
            @pl.when(bit(kvs, p))
            def _():
                pltpu.make_async_copy(kvrecv.at[u, p], kvbuf.at[slot, p], kvsem.at[slot, p]).wait()

            @pl.when(bit(qs, p))
            def _():
                pltpu.make_async_copy(qrecv.at[u, p], qbuf.at[slot, p], qsem.at[slot, p]).wait()

        ones = jnp.ones((8, own), jnp.bfloat16)

        def lowest(mask):
            return _first([(lax.shift_right_logical(mask, jnp.int32(b)) & 1) == 1 for b in range(n)])

        def block(some, j, diagonal=False):
            scores, weights, keeps = [], [], []
            for h in range(TWO):
                keys = [kvbuf[slot, i, 0, h] for i in some]
                scores.append(_dot(jnp.concatenate(keys, axis=0) if len(some) > 1 else keys[0], qbuf[slot, j, h], 1, 1))
            for h, s in enumerate(scores):
                if diagonal:
                    seen = lax.broadcasted_iota(jnp.int32, s.shape, 1) >= lax.broadcasted_iota(jnp.int32, s.shape, 0)
                    s = jnp.where(seen, s, NEG)
                old = top[h]
                best = jnp.maximum(old, s.max(axis=0, keepdims=True))
                top[h] = best
                weights.append(jnp.exp2((s - best) * e).astype(jnp.bfloat16))
                keeps.append(jnp.exp2((old - best) * e))
            for h in range(TWO):
                values = []
                for i in some:
                    v = kvbuf[slot, i, 1, h]
                    values += [v[:HEAD], v[HEAD:]]
                values = jnp.concatenate([jnp.concatenate(values, axis=1)] + [jnp.concatenate([ones] * len(some), axis=1)], axis=0)
                mix[h] = mix[h] * keeps[h] + _dot(values, weights[h], 1, 0)

        def mine(j):
            return start + count(qs & ((1 << j) - 1))

        def send_back(j):
            place = sum((lax.shift_right_logical(m, j) & 1) << b for b, m in enumerate(places))
            pltpu.make_async_remote_copy(
                src_ref=ostage.at[mine(j)], dst_ref=orecv.at[u, place], send_sem=ossem.at[u], recv_sem=orsem.at[u],
                device_id=to(j), device_id_type=MESH).start()
            pltpu.make_async_remote_copy(
                src_ref=lstage.at[mine(j)], dst_ref=lrecv.at[u, place], send_sem=lssem.at[u], recv_sem=lrsem.at[u],
                device_id=to(j), device_id_type=MESH).start()

        def meet(j, mask):
            many = count(mask)

            def several(number):
                def go(_, mask):
                    some = []
                    for _ in range(number):
                        some.append(lowest(mask))
                        mask = mask & (mask - 1)
                    block(some, j)
                    return mask

                return go

            mask = lax.fori_loop(0, lax.div(many, 4), several(4), mask)
            mask = lax.fori_loop(0, lax.div(lax.rem(many, 4), 2), several(2), mask)

            @pl.when(lax.rem(many, 2) == 1)
            def _():
                block([lowest(mask)], j)

        def clear():
            top[...] = jnp.full_like(top, NEG)
            mix[...] = jnp.zeros_like(mix)

        def job(_, state):
            left, last = state
            j = lowest(left)
            clear()
            meet(j, _choose(j, masks))

            @pl.when(last >= 0)
            def _():
                send_back(last)

            slot = mine(j)
            for h in range(TWO):
                total = mix[h, HEAD : HEAD + 1, :]
                ostage[slot, h] = (mix[h, :HEAD, :] * (1 / total)).astype(jnp.bfloat16)
                lstage[slot, h : h + 1, :] = top[h] * e + jnp.log(total) * LOG2E
            return left & (left - 1), j

        _, last = lax.fori_loop(0, number, job, (qs, jnp.int32(-1)))
        clear()
        block([me], me, True)

        @pl.when(last >= 0)
        def _():
            send_back(last)

        meet(me, _choose(me, masks) & ~(1 << me))
        ltop[kept] = top[...]
        lmix[kept] = mix[...]

    def sent(u):
        c = kind(u)
        away = count(look(plan.q_from, c))
        await_many(stage.at[:, 0], ssem.at[u], 2 * count(look(plan.kv_to, c)) + count(look(plan.q_to, c)), 3 * (n - 1))
        await_many(ostage, ossem.at[u], away, n - 1)
        await_many(lstage, lssem.at[u], away, n - 1)

    def finish(u):
        c, kept = kind(u), lax.rem(u, KEPT)
        number = count(look(plan.q_to, c))
        await_many(orecv.at[u], orsem.at[u], number, plan.most)
        await_many(lrecv.at[u], lrsem.at[u], number, plan.most)
        for parts in range(plan.most + 1):
            @pl.when(number == parts)
            def _():
                for h in range(TWO):
                    base = ltop[kept, h] * e
                    logs = [lrecv[u, r, h : h + 1, :] for r in range(parts)]
                    best = functools.reduce(jnp.maximum, logs, base)
                    keep = jnp.exp2(base - best)
                    total = lmix[kept, h, HEAD : HEAD + 1, :] * keep
                    out = lmix[kept, h, :HEAD, :] * keep
                    for r in range(parts):
                        w = jnp.exp2(logs[r] - best)
                        total += w
                        out += orecv[u, r, h].astype(jnp.float32) * w
                    obuf[:, h * HEAD : (h + 1) * HEAD] = (out * (1 / total)).T.astype(jnp.bfloat16)

        load_out(u).wait()
        slot = lax.rem(u, 2)

        @pl.when(u == 0)
        def _():
            for at in range(0, d, TILE):
                y[:, at : at + TILE] = _dot(obuf[...], wobuf[slot, :, at : at + TILE], 1, 0)

        @pl.when((u > 0) & (u < units - 1))
        def _():
            for at in range(0, d, TILE):
                y[:, at : at + TILE] += _dot(obuf[...], wobuf[slot, :, at : at + TILE], 1, 0)

        @pl.when(u == units - 1)
        def _():
            for b in range(blocks):
                getx(b).wait()
            for at in range(0, d, TILE):
                got = y[:, at : at + TILE] + _dot(obuf[...], wobuf[slot, :, at : at + TILE], 1, 0)
                a[:, at : at + TILE] = (a[:, at : at + TILE].astype(jnp.float32) + got).astype(jnp.bfloat16)

    def step(it, _):
        @pl.when((it >= BACK - 1) & (it < units + BACK - 1))
        def _():
            load_out(it - (BACK - 1)).start()

        @pl.when(it < units)
        def _():
            lax.fori_loop(0, 3, multiply, it)
            across(it)

        @pl.when(it == units)
        def _():
            keep(3 * it - 1)

        @pl.when((it > 0) & (it <= units))
        def _():
            send_q(it - 1)

        @pl.when(it == units)
        def _():
            for b in range(blocks):
                getx(b).start()

        @pl.when(it < units)
        def _():
            send_kv(it, 1)

        @pl.when((it >= LAG) & (it < units + LAG))
        def _():
            attend(it - LAG)

        @pl.when(it >= BACK)
        def _():
            finish(it - BACK)

        @pl.when(it >= BACK + LATE)
        def _():
            sent(it - (BACK + LATE))

        @pl.when((it >= LAG - 1) & (it < units + LAG - 1))
        def _():
            fetch(it - (LAG - 1))

        return 0

    lax.fori_loop(0, units + BACK, step, 0)

    for u in range(units - LATE, units):
        sent(jnp.int32(u))


def solution(mesh):
    n = mesh.shape["sp"]

    def step(x, gain, wq, wk, wv, wo):
        own, d = x.shape
        units = wq.shape[1] // TILE
        plan = Plan(n)
        half = HEAD // 2
        place = lax.axis_index("sp") * own + jnp.arange(own)
        angle = place.astype(jnp.float32)[:, None] * THETA ** (-jnp.arange(half, dtype=jnp.float32) / half)
        cos, sin = jnp.cos(angle), jnp.sin(angle)
        blocks = 4
        hbm, vmem = pl.BlockSpec(memory_space=pl.ANY), pl.BlockSpec(memory_space=pltpu.VMEM)
        bf16, f32 = jnp.bfloat16, jnp.float32
        dma = pltpu.SemaphoreType.DMA
        return pl.pallas_call(
            functools.partial(_kernel, n, units, plan),
            name="layer",
            out_shape=[
                pltpu.VMEM((own, d), bf16),
                jax.ShapeDtypeStruct((units, n, 2, TWO, own, HEAD), bf16),
                jax.ShapeDtypeStruct((units, n, TWO, own, HEAD), bf16),
            ],
            in_specs=[hbm, vmem, vmem, vmem, hbm, hbm, hbm, hbm],
            out_specs=[vmem, hbm, hbm],
            scratch_shapes=[
                pltpu.VMEM((3, d, TILE), bf16),
                pltpu.VMEM((2, TILE, d), bf16),
                pltpu.VMEM((units, 3, TWO, own, HEAD), bf16),
                pltpu.VMEM((2, n, 2, TWO, own, HEAD), bf16),
                pltpu.VMEM((2, n, TWO, own, HEAD), bf16),
                pltpu.VMEM((TWO, 1, own), f32),
                pltpu.VMEM((TWO, HEAD + 8, own), f32),
                pltpu.VMEM((KEPT, TWO, 1, own), f32),
                pltpu.VMEM((KEPT, TWO, HEAD + 8, own), f32),
                pltpu.VMEM((plan.held, TWO, HEAD, own), bf16),
                pltpu.VMEM((plan.held, TWO, own), f32),
                pltpu.VMEM((units, plan.most, TWO, HEAD, own), bf16),
                pltpu.VMEM((units, plan.most, TWO, own), f32),
                pltpu.VMEM((own, TILE), bf16),
                pltpu.VMEM((own, d), f32),
                pltpu.VMEM((2, own, TILE), f32),
                pltpu.VMEM((2, 2, own, HEAD), f32),
                dma((5,)), dma((blocks,)), dma((units,)), dma((units,)), dma((2, n)), dma((2, n)),
                dma((units,)), dma((units,)), dma((units,)), dma((units,)),
            ],
            compiler_params=pltpu.CompilerParams(collective_id=0, has_side_effects=True, vmem_limit_bytes=63300000),
        )(x, gain.reshape(d // HEAD, HEAD), cos, sin, wq, wk, wv, wo)[0]

    tokens, whole = P(("dp", "sp"), None), P(None, None)
    return jax.shard_map(
        step,
        mesh=mesh,
        in_specs=(tokens, P(None), whole, whole, whole, whole),
        out_specs=tokens,
        check_vma=False,
    )
```
